8 devices in a mesh: col: 4 (over z, y, x), row: 2 (over core).
Axes of the slice: x: 2, y: 2, z: 1, core: 2. Of those that a mesh axis runs over, the one named last changes fastest.
Arguments:
- vel_u: float32 [31, 512, 2048], P(None, 'row', 'col')
- vel_v: float32 [31, 512, 2048], P(None, 'row', 'col')
- temperature: float32 [31, 512, 2048], P(None, 'row', 'col')
- salinity: float32 [31, 512, 2048], P(None, 'row', 'col')
- sea_level: float32 [512, 2048], P('row', 'col')
- trans_u: float32 [512, 2048], P('row', 'col')
- trans_v: float32 [512, 2048], P('row', 'col')
- bathymetry: float32 [512, 2048], P('row', 'col')
- kmt_levels: int32 [512, 2048], P('row', 'col')
- tide_force: float32 [30, 2], replicated
Outputs:
- output 1: float32 [512, 2048], P('row', 'col')
- output 2: float32 [512, 2048], P('row', 'col')
- output 3: float32 [512, 2048], P('row', 'col')
- output 4: float32 [31, 512, 2048], P(None, 'row', 'col')
- output 5: float32 [31, 512, 2048], P(None, 'row', 'col')
- output 6: float32 [31, 512, 2048], P(None, 'row', 'col')
- output 7: float32 [31, 512, 2048], P(None, 'row', 'col')
All inputs are finite; a program needn't handle non-finite values.
Results may differ from the reference program's by a relative error of at most 0.001.
Values sent between devices are 32-bit elements.
A program may use at most 1 GiB of HBM per device.

```python
import jax
import jax.numpy as jnp
from jax import lax

LEVELS = 31
SUBCYCLES = 30
GRID_NY = 512
GRID_NX = 2048

GRAVITY = 1.0
GRID_DX = 1.0
TIME_STEP = 4.0
ALPHA_T = 0.02
BETA_S = 0.015
T_REF = 1.0
S_REF = 1.0
VISC_KV = 0.001
DIFF_KT = 0.0005


def pad_halo(field):
    wrapped = jnp.concatenate([field[..., -1:], field, field[..., :1]], axis=-1)
    walls = jnp.zeros_like(wrapped[..., :1, :])
    return jnp.concatenate([walls, wrapped, walls], axis=-2)


def level_mask(count, n_levels):
    levels = jnp.arange(n_levels, dtype=jnp.int32)[:, None, None]
    return (levels < count[None]).astype(jnp.float32)


def interface_coef(count, thick, kappa, n_levels):
    levels = jnp.arange(n_levels - 1, dtype=jnp.int32)[:, None, None]
    active = (levels + 1 < count[None]).astype(jnp.float32)
    safe = jnp.where(count > 0, thick, 1.0)
    return active * (TIME_STEP * kappa / (safe * safe))[None]


def column_solve(source, couple):
    edge = jnp.zeros_like(source[:1])
    upper = jnp.concatenate([couple, edge], axis=0)
    lower = jnp.concatenate([edge, couple], axis=0)
    diag = 1.0 + upper + lower

    def forward(carry, slab):
        gain_prev, part_prev = carry
        lower_k, diag_k, upper_k, source_k = slab
        pivot = diag_k - lower_k * gain_prev
        gain = upper_k / pivot
        part = (source_k + lower_k * part_prev) / pivot
        return (gain, part), (gain, part)

    start = (jnp.zeros_like(source[0]), jnp.zeros_like(source[0]))
    _, (gains, parts) = lax.scan(forward, start, (lower, diag, upper, source))

    def backward(below, slab):
        gain, part = slab
        here = part + gain * below
        return here, here

    _, profile = lax.scan(backward, jnp.zeros_like(source[0]), (gains, parts), reverse=True)
    return profile


def geometry(kmt_ext, depth_ext):
    kmt_cell = kmt_ext[1:-1, 1:-1]
    thick_ext = depth_ext / jnp.maximum(kmt_ext, 1).astype(jnp.float32)
    thick_cell = thick_ext[1:-1, 1:-1]
    return {"k_cell": kmt_cell, "k_u": jnp.minimum(kmt_cell, kmt_ext[1:-1, 2:]), "k_v": jnp.minimum(kmt_cell, kmt_ext[2:, 1:-1]), "dz_cell": thick_cell, "dz_u": 0.5 * (thick_cell + thick_ext[1:-1, 2:]), "dz_v": 0.5 * (thick_cell + thick_ext[2:, 1:-1])}


def surface_fields(layout):
    k_faces = jnp.stack([layout["k_u"], layout["k_v"]])
    face_depth = k_faces.astype(jnp.float32) * jnp.stack([layout["dz_u"], layout["dz_v"]])
    face_wet = (k_faces > 0).astype(jnp.float32)
    wet_cell = (layout["k_cell"] > 0).astype(jnp.float32)
    return face_depth, face_wet, wet_cell


def momentum_tend(u_ext, v_ext, p_ext):
    cen_u = 0.5 * (u_ext[:, 1:-1, :-1] + u_ext[:, 1:-1, 1:])
    corner_v = 0.5 * (v_ext[:, :-1, 1:-1] + v_ext[:, :-1, 2:])
    corner_u = 0.5 * (u_ext[:, :-1, 1:-1] + u_ext[:, 1:, 1:-1])
    flux_uu = cen_u * cen_u
    flux_vu = corner_v * corner_u
    tend_u = -(flux_uu[:, :, 1:] - flux_uu[:, :, :-1] + flux_vu[:, 1:, :] - flux_vu[:, :-1, :] + p_ext[:, 1:-1, 2:] - p_ext[:, 1:-1, 1:-1]) / GRID_DX
    cen_v = 0.5 * (v_ext[:, :-1, 1:-1] + v_ext[:, 1:, 1:-1])
    side_u = 0.5 * (u_ext[:, 1:-1, :-1] + u_ext[:, 2:, :-1])
    side_v = 0.5 * (v_ext[:, 1:-1, :-1] + v_ext[:, 1:-1, 1:])
    flux_vv = cen_v * cen_v
    flux_uv = side_u * side_v
    tend_v = -(flux_vv[:, 1:, :] - flux_vv[:, :-1, :] + flux_uv[:, :, 1:] - flux_uv[:, :, :-1] + p_ext[:, 2:, 1:-1] - p_ext[:, 1:-1, 1:-1]) / GRID_DX
    return tend_u, tend_v


def baroclinic_predict(vel_u, vel_v, temperature, salinity, layout, halo_fn):
    n_levels = vel_u.shape[0]
    mask_c = level_mask(layout["k_cell"], n_levels)
    mask_u = level_mask(layout["k_u"], n_levels)
    mask_v = level_mask(layout["k_v"], n_levels)
    vel_um = vel_u * mask_u
    vel_vm = vel_v * mask_v
    density = mask_c * (BETA_S * (salinity - S_REF) - ALPHA_T * (temperature - T_REF))
    pressure = GRAVITY * layout["dz_cell"] * (jnp.cumsum(density, axis=0) - 0.5 * density)
    cell_coef = interface_coef(layout["k_cell"], layout["dz_cell"], DIFF_KT, n_levels)
    temp_mix = column_solve(temperature * mask_c, cell_coef)
    salt_mix = column_solve(salinity * mask_c, cell_coef)
    edges = halo_fn(jnp.stack([vel_um, vel_vm, pressure, temp_mix, salt_mix]))
    tend_u, tend_v = momentum_tend(edges[0], edges[1], edges[2])
    u_star = column_solve(mask_u * (vel_um + TIME_STEP * tend_u), interface_coef(layout["k_u"], layout["dz_u"], VISC_KV, n_levels))
    v_star = column_solve(mask_v * (vel_vm + TIME_STEP * tend_v), interface_coef(layout["k_v"], layout["dz_v"], VISC_KV, n_levels))
    forcing = jnp.stack([jnp.sum(layout["dz_u"] * (u_star - vel_um), axis=0), jnp.sum(layout["dz_v"] * (v_star - vel_vm), axis=0)]) / TIME_STEP
    return u_star, v_star, forcing, edges[3:], (mask_c, mask_u, mask_v)


def barotropic(eta_start, trans_start, face_depth, face_wet, wet_cell, forcing, tide_force, halo_fn):
    n_sub = tide_force.shape[0]
    dt_sub = TIME_STEP / n_sub
    weight_norm = 6.0 / (n_sub * (n_sub + 1) * (n_sub + 2))

    def substep(step, carry):
        eta_now, trans_now, trans_avg = carry
        trans_ext = halo_fn(trans_now)
        divergence = (trans_now[0] - trans_ext[0, 1:-1, :-2] + trans_now[1] - trans_ext[1, :-2, 1:-1]) / GRID_DX
        eta_next = wet_cell * (eta_now - dt_sub * divergence)
        eta_ext = halo_fn(eta_next)
        slope = jnp.stack([eta_ext[1:-1, 2:] - eta_next, eta_ext[2:, 1:-1] - eta_next]) / GRID_DX
        tide_now = lax.dynamic_index_in_dim(tide_force, step, 0, keepdims=False)
        trans_next = face_wet * (trans_now + dt_sub * (face_depth * (tide_now[:, None, None] - GRAVITY * slope) + forcing))
        weight = weight_norm * ((step + 1) * (n_sub - step)).astype(jnp.float32)
        return eta_next, trans_next, trans_avg + weight * trans_next

    return lax.fori_loop(0, n_sub, substep, (eta_start, trans_start, jnp.zeros_like(trans_start)))


def correct_velocity(star, dz_face, depth_face, mean_trans, mask):
    safe = jnp.where(depth_face > 0, depth_face, 1.0)
    return mask * (star + ((mean_trans - jnp.sum(dz_face * star, axis=0)) / safe)[None])


def advect_tracers(tracer_ext, flow_ext, mask_c):
    flux_x = flow_ext[0, :, 1:-1, :-1] * (0.5 * (tracer_ext[..., 1:-1, :-1] + tracer_ext[..., 1:-1, 1:]))
    flux_y = flow_ext[1, :, :-1, 1:-1] * (0.5 * (tracer_ext[..., :-1, 1:-1] + tracer_ext[..., 1:, 1:-1]))
    divergence = (flux_x[..., 1:] - flux_x[..., :-1] + flux_y[..., 1:, :] - flux_y[..., :-1, :]) / GRID_DX
    return mask_c * (tracer_ext[..., 1:-1, 1:-1] - TIME_STEP * divergence)


def baroclinic_finish(u_star, v_star, trans_avg, face_depth, layout, tracer_ext, masks, halo_fn):
    mask_c, mask_u, mask_v = masks
    vel_uc = correct_velocity(u_star, layout["dz_u"], face_depth[0], trans_avg[0], mask_u)
    vel_vc = correct_velocity(v_star, layout["dz_v"], face_depth[1], trans_avg[1], mask_v)
    flows = halo_fn(jnp.stack([vel_uc, vel_vc]))
    tracers = advect_tracers(tracer_ext, flows, mask_c)
    return vel_uc, vel_vc, tracers[0], tracers[1]


def ocean_step(vel_u, vel_v, temperature, salinity, sea_level, trans_u, trans_v, bathymetry, kmt_levels, tide_force, halo_fn):
    layout = geometry(halo_fn(kmt_levels), halo_fn(bathymetry))
    u_star, v_star, forcing, tracer_ext, masks = baroclinic_predict(vel_u, vel_v, temperature, salinity, layout, halo_fn)
    face_depth, face_wet, wet_cell = surface_fields(layout)
    eta_new, trans_new, trans_avg = barotropic(wet_cell * sea_level, face_wet * jnp.stack([trans_u, trans_v]), face_depth, face_wet, wet_cell, forcing, tide_force, halo_fn)
    vel_uc, vel_vc, temp_new, salt_new = baroclinic_finish(u_star, v_star, trans_avg, face_depth, layout, tracer_ext, masks, halo_fn)
    return eta_new, trans_new[0], trans_new[1], vel_uc, vel_vc, temp_new, salt_new


def draw_levels(key):
    key_count, key_land = jax.random.split(key)
    counts = jax.random.randint(key_count, (GRID_NY, GRID_NX), (LEVELS + 2) // 3, LEVELS + 1)
    land = jax.random.randint(key_land, (GRID_NY, GRID_NX), 0, 12) == 0
    levels = jnp.where(land, 0, counts).astype(jnp.int32)
    return levels.at[0, 0].set(0).at[GRID_NY - 1, GRID_NX - 1].set(LEVELS)


def setup_inputs(seed: int = 0) -> dict:
    keys = jax.random.split(jax.random.key(seed), 10)
    shape_cube = (LEVELS, GRID_NY, GRID_NX)
    shape_plane = (GRID_NY, GRID_NX)
    depth_frac = jnp.arange(LEVELS, dtype=jnp.float32)[:, None, None] / LEVELS
    return {
        "vel_u": 0.1 * jax.random.normal(keys[0], shape_cube, jnp.float32),
        "vel_v": 0.1 * jax.random.normal(keys[1], shape_cube, jnp.float32),
        "temperature": 2.0 * (1.0 - depth_frac) + 0.5 * jax.random.normal(keys[2], shape_cube, jnp.float32),
        "salinity": 1.0 + depth_frac + 0.3 * jax.random.normal(keys[3], shape_cube, jnp.float32),
        "sea_level": 0.05 * jax.random.normal(keys[4], shape_plane, jnp.float32),
        "trans_u": 0.05 * jax.random.normal(keys[5], shape_plane, jnp.float32),
        "trans_v": 0.05 * jax.random.normal(keys[6], shape_plane, jnp.float32),
        "bathymetry": 0.6 + 0.8 * jax.random.uniform(keys[7], shape_plane, jnp.float32),
        "kmt_levels": draw_levels(keys[8]),
        "tide_force": 0.01 + 0.01 * jax.random.normal(keys[9], (SUBCYCLES, 2), jnp.float32),
    }


def reference(vel_u, vel_v, temperature, salinity, sea_level, trans_u, trans_v, bathymetry, kmt_levels, tide_force):
    return ocean_step(vel_u, vel_v, temperature, salinity, sea_level, trans_u, trans_v, bathymetry, kmt_levels, tide_force, pad_halo)
```

```python
import functools

import jax
import jax.numpy as jnp
from jax import lax
from jax.experimental import pallas as pl
from jax.experimental.pallas import tpu as pltpu
from jax.sharding import PartitionSpec as P

MESH = pl.DeviceIdType.MESH
F32 = jnp.float32

TIME_STEP = 4.0
ALPHA_T = 0.02
BETA_S = 0.015
T_REF = 1.0
S_REF = 1.0
VISC_KV = 0.001
DIFF_KT = 0.0005

LANE = 128
LAST = LANE - 1
PAIR = 64
TAIL = 96
TILE = 8
STRIP = 32
MID = 40
ZERO = 0.0

NK = 31
NR = 256
NX = 512
NP = 4
RB = 32
NB = NR // RB
HALO = 32
ER = NR + HALO
VMEM_LIMIT = 62 * 1024 * 1024

ANY = pl.BlockSpec(memory_space=pl.ANY)
WHOLE = pl.BlockSpec(memory_space=pltpu.VMEM)


def lanes_of(shape):
    return lax.broadcasted_iota(jnp.int32, shape, len(shape) - 1)


def roll_to(x, source, target):
    return pltpu.roll(x, lax.rem(target - source + 256, LANE), x.ndim - 1)


def shift_east(planes):
    lane = lanes_of(planes[0].shape)
    rolled = [pltpu.roll(x, LAST, x.ndim - 1) for x in planes]
    return [jnp.where(lane == LAST, rolled[(n + 1) % len(planes)], rolled[n]) for n in range(len(planes))]


def shift_west(planes):
    lane = lanes_of(planes[0].shape)
    rolled = [pltpu.roll(x, 1, x.ndim - 1) for x in planes]
    return [jnp.where(lane == 0, rolled[n - 1], rolled[n]) for n in range(len(planes))]


def mix_kernel(t_ref, s_ref, uw_ref, ue_ref, vw_ref, ve_ref, kmt_ref, h_ref, eta_ref, tu_ref, tv_ref,
               p_out, t_out, s_out, ewa_out, eea_out, ewb_out, eeb_out, p1w_out, p1e_out,
               gain_s, pt_s, ps_s):

    def group(g, _):
        rows = pl.ds(pl.multiple_of(TILE * g, TILE), TILE)
        kf = kmt_ref[rows, :].astype(F32)
        dz = h_ref[rows, :] / jnp.maximum(kf, 1.0)
        safe = jnp.where(kf > 0, dz, 1.0)
        coef = (TIME_STEP * DIFF_KT) / (safe * safe)
        dz4 = 4.0 * dz
        zero = jnp.zeros_like(dz)
        cum, gain, pt, ps, low = zero, zero, zero, zero, zero
        for k in range(NK):
            wet = kf > k
            t = t_ref[k, rows, :]
            s = s_ref[k, rows, :]
            dens = jnp.where(wet, BETA_S * (s - S_REF) - ALPHA_T * (t - T_REF), ZERO)
            cum = cum + dens
            p4 = dz4 * (cum - 0.5 * dens)
            for l in range(NP):
                p_out[k, l, rows, :] = p4[:, LANE * l:LANE * l + LANE]
            up = jnp.where(kf > k + 1, coef, ZERO) if k < NK - 1 else zero
            inv = 1.0 / ((1.0 + up + low) - low * gain)
            gain = up * inv
            pt = (jnp.where(wet, t, ZERO) + low * pt) * inv
            ps = (jnp.where(wet, s, ZERO) + low * ps) * inv
            gain_s[k] = gain
            pt_s[k] = pt
            ps_s[k] = ps
            low = up
        bt, bs = zero, zero
        for k in range(NK - 1, -1, -1):
            gain = gain_s[k]
            bt = pt_s[k] + gain * bt
            bs = ps_s[k] + gain * bs
            for l in range(NP):
                t_out[k, l, rows, :] = bt[:, LANE * l:LANE * l + LANE]
                s_out[k, l, rows, :] = bs[:, LANE * l:LANE * l + LANE]
        return 0

    lax.fori_loop(0, RB // TILE, group, 0)

    lane = lanes_of((RB, LANE))

    def pack(k, carry):
        ewa, eea, ewb = carry
        for f, x in enumerate((uw_ref[k], vw_ref[k], p_out[k, 0], t_out[k, 0])):
            ewa = jnp.where(lane == STRIP * f + k, roll_to(x, 0, STRIP * f + k), ewa)
        for f, x in enumerate((ue_ref[k], ve_ref[k], t_out[k, 3], s_out[k, 3])):
            eea = jnp.where(lane == STRIP * f + k, roll_to(x, LAST, STRIP * f + k), eea)
        ewb = jnp.where(lane == STRIP + k, roll_to(s_out[k, 0], 0, STRIP + k), ewb)
        return ewa, eea, ewb

    zero = jnp.zeros((RB, LANE), F32)
    kf = kmt_ref[...].astype(F32)
    ewa, eea, ewb = lax.fori_loop(0, NK, pack, (zero, zero, zero))
    ewa_out[...] = ewa
    eea_out[...] = eea
    ewb_out[...] = jnp.where(lane < STRIP, kf[:, :LANE], ewb)
    eeb_out[...] = jnp.where(lane < STRIP, pltpu.roll(kf[:, 384:], STRIP, 1), ZERO)
    west, east = zero, zero
    for f, ref in enumerate((eta_ref, tu_ref, tv_ref, h_ref)):
        mine = (lane >= STRIP * f) & (lane < STRIP * f + STRIP)
        west = jnp.where(mine, pltpu.roll(ref[:, :LANE], STRIP * f, 1) if f else ref[:, :LANE], west)
        spun = (STRIP * f + STRIP) % LANE
        east = jnp.where(mine, pltpu.roll(ref[:, 384:], spun, 1) if spun else ref[:, 384:], east)
    p1w_out[...] = west
    p1e_out[...] = east


def mix(vel_u, vel_v, temp, salt, eta, trans_u, trans_v, depth, kmt):
    cube = pl.BlockSpec((NK, RB, NX), lambda r: (0, r, 0))
    west = pl.BlockSpec((NK, RB, LANE), lambda r: (0, r, 0))
    east = pl.BlockSpec((NK, RB, LANE), lambda r: (0, r, 3))
    plane = pl.BlockSpec((RB, NX), lambda r: (r, 0))
    out_cube = pl.BlockSpec((NK, NP, RB, LANE), lambda r: (0, 0, r, 0))
    edge = pl.BlockSpec((RB, LANE), lambda r: (r, 0))
    cubes = jax.ShapeDtypeStruct((NK, NP, NR, LANE), F32)
    edges = jax.ShapeDtypeStruct((NR, LANE), F32)
    return pl.pallas_call(
        mix_kernel,
        grid=(NB,),
        in_specs=[cube, cube, west, east, west, east, plane, plane, plane, plane, plane],
        out_specs=[out_cube] * 3 + [edge] * 6,
        out_shape=[cubes] * 3 + [edges] * 6,
        scratch_shapes=[pltpu.VMEM((NK, TILE, NX), F32)] * 3,
        compiler_params=pltpu.CompilerParams(vmem_limit_bytes=VMEM_LIMIT),
        name="mix",
    )(temp, salt, vel_u, vel_u, vel_v, vel_v, kmt, depth, eta, trans_u, trans_v)


def exchange_kernel(plan, n_cols, n_in, *refs):
    ins, outs = refs[:n_in], refs[n_in:-2]
    send_sem, recv_sem = refs[-2:]
    col, row = lax.axis_index("col"), lax.axis_index("row")
    west = lax.rem(col + n_cols - 1, n_cols)
    east = lax.rem(col + 1, n_cols)
    other = 1 - row
    peers = [(west, row), (east, row), (col, other), (west, other), (east, other)]
    barrier = pltpu.get_barrier_semaphore()
    for peer in peers:
        pl.semaphore_signal(barrier, inc=1, device_id=peer, device_id_type=MESH)
    pl.semaphore_wait(barrier, len(peers))

    copies = []

    def send(src, dst, peer):
        n = len(copies)
        copies.append(pltpu.make_async_remote_copy(
            src_ref=src, dst_ref=dst, send_sem=send_sem.at[n], recv_sem=recv_sem.at[n],
            device_id=peer, device_id_type=MESH))
        copies[-1].start()

    for kind, i, o, depth in plan:
        src, dst = ins[i], outs[o]
        start = pl.multiple_of((1 - row) * (NR - depth), TILE)
        if kind in ("west", "east"):
            to = west if kind == "west" else east
            send(src, dst.at[pl.ds(0, NR)], (to, row))
            if depth:
                send(src.at[pl.ds(start, depth)], dst.at[pl.ds(NR, depth)], (to, other))
        elif kind == "rows2":
            send(src.at[pl.ds(start, depth)], dst, (col, other))
        elif kind == "rows3":
            send(src.at[:, pl.ds(start, depth)], dst, (col, other))
        else:
            send(src.at[:, :, pl.ds(start, depth)], dst, (col, other))
    for copy in copies:
        copy.wait()


def exchange(n_cols, plan, ins, out_shapes, ident):
    n = sum(2 if kind in ("west", "east") and depth else 1 for kind, _, _, depth in plan)
    return pl.pallas_call(
        functools.partial(exchange_kernel, plan, n_cols, len(ins)),
        in_specs=[ANY] * len(ins),
        out_specs=[ANY] * len(out_shapes),
        out_shape=out_shapes,
        scratch_shapes=[pltpu.SemaphoreType.DMA((n,)), pltpu.SemaphoreType.DMA((n,))],
        compiler_params=pltpu.CompilerParams(collective_id=ident, has_side_effects=True),
        name=f"exchange{ident}",
    )(*ins)


def halo_tile(from_east, from_west, field):
    lane = lanes_of(from_east.shape)
    spun = (LANE - STRIP * field) % LANE
    e = pltpu.roll(from_east, spun, 1) if spun else from_east
    spun = (TAIL - STRIP * field) % LANE
    w = pltpu.roll(from_west, spun, 1) if spun else from_west
    return jnp.where(lane < STRIP, e, jnp.where(lane >= TAIL, w, ZERO))


def geometry_kernel(kmt_ref, h_ref, eta_ref, tu_ref, tv_ref, rep_ref, rwp_ref, reb_ref, rwb_ref,
                    rk_ref, rh_ref, reta_ref, rtu_ref, rtv_ref,
                    ku_out, kv_out, dzu_out, dzv_out, kc_out, eta_out, tu_out, tv_out, k_s, dz_s):
    row = lax.axis_index("row")

    def fill(c, _):
        rows = pl.ds(pl.multiple_of(RB * c, TILE), RB)

        def put(l, kf, h):
            k_s[l, rows, :] = kf
            dz_s[l, rows, :] = h / jnp.maximum(kf, 1.0)

        k_tile = halo_tile(reb_ref[rows, :], rwb_ref[rows, :], 0)
        h_tile = halo_tile(rep_ref[rows, :], rwp_ref[rows, :], 3)

        @pl.when(c < NB)
        def _():
            for l in range(NP):
                cut = slice(LANE * l, LANE * l + LANE)
                put(l, kmt_ref[rows, cut].astype(F32), h_ref[rows, cut])
                eta_out[l, rows, :] = eta_ref[rows, cut]
                tu_out[l, rows, :] = tu_ref[rows, cut]
                tv_out[l, rows, :] = tv_ref[rows, cut]

        @pl.when(c == NB)
        def _():
            for l in range(NP):
                cut = slice(LANE * l, LANE * l + LANE)
                put(l, rk_ref[:, cut].astype(F32), rh_ref[:, cut])
                eta_out[l, rows, :] = reta_ref[:, cut]
                tu_out[l, rows, :] = rtu_ref[:, cut]
                tv_out[l, rows, :] = rtv_ref[:, cut]

        put(NP, k_tile, h_tile)
        for f, out in enumerate((eta_out, tu_out, tv_out)):
            out[NP, rows, :] = halo_tile(rep_ref[rows, :], rwp_ref[rows, :], f)
        return 0

    lax.fori_loop(0, ER // RB, fill, 0)
    k_s[:, ER:ER + TILE, :] = k_s[:, 0:TILE, :]
    dz_s[:, ER:ER + TILE, :] = dz_s[:, 0:TILE, :]
    cut_row = jnp.where(row == 0, ER - 1, NR - 1)

    for c in range(ER // RB):
        base = RB * c
        rows = slice(base, base + RB)
        north = slice(base + 1, base + RB + 1)
        k = [k_s[l, rows, :] for l in range(NP + 1)]
        dz = [dz_s[l, rows, :] for l in range(NP + 1)]
        k_e = shift_east(k)
        dz_e = shift_east(dz)
        at = lax.broadcasted_iota(jnp.int32, (RB, LANE), 0) + base
        for l in range(NP + 1):
            ku = jnp.minimum(k[l], k_e[l])
            kv = jnp.where(at == cut_row, ZERO, jnp.minimum(k[l], k_s[l, north, :]))
            ku_out[l, rows, :] = ku
            kv_out[l, rows, :] = kv
            kc_out[l, rows, :] = k[l]
            dzu_out[l, rows, :] = 0.5 * (dz[l] + dz_e[l])
            dzv_out[l, rows, :] = 0.5 * (dz[l] + dz_s[l, north, :])
            eta_out[l, rows, :] = jnp.where(k[l] > 0, eta_out[l, rows, :], ZERO)
            tu_out[l, rows, :] = jnp.where(ku > 0, tu_out[l, rows, :], ZERO)
            tv_out[l, rows, :] = jnp.where(kv > 0, tv_out[l, rows, :], ZERO)


def geometry(*args):
    out = jax.ShapeDtypeStruct((NP + 1, ER, LANE), F32)
    return pl.pallas_call(
        geometry_kernel,
        in_specs=[WHOLE] * len(args),
        out_specs=[WHOLE] * TILE,
        out_shape=[out] * TILE,
        scratch_shapes=[pltpu.VMEM((NP + 1, ER + TILE, LANE), F32)] * 2,
        compiler_params=pltpu.CompilerParams(vmem_limit_bytes=VMEM_LIMIT),
        name="geometry",
    )(*args)


def window_copies(src, halo, buf, sem, r, slot, start):
    def piece(ref, lo, n, at, which):
        if len(ref.shape) == 4:
            pairs = [(ref.at[:, :, pl.ds(lo, n)], buf.at[slot, :, pl.ds(0, NP), pl.ds(at, n)])]
        else:
            pairs = [(ref.at[:, pl.ds(lo, n), pl.ds(LANE * l, LANE)], buf.at[slot, :, l, pl.ds(at, n)])
                     for l in range(NP)]
        for a, b in pairs:
            copy = pltpu.make_async_copy(a, b, sem.at[slot])
            if start:
                copy.start()
            else:
                copy.wait()

    piece(src, pl.multiple_of(RB * r, TILE), RB, TILE, 0)
    if start:
        @pl.when(r == 0)
        def _():
            piece(halo, 0, TILE, 0, 1)

        @pl.when(r > 0)
        def _():
            piece(src, pl.multiple_of(RB * r - TILE, TILE), TILE, 0, 1)

        @pl.when(r == NB - 1)
        def _():
            piece(halo, 0, TILE, RB + TILE, 2)

        @pl.when(r < NB - 1)
        def _():
            piece(src, pl.multiple_of(RB * r + RB, TILE), TILE, RB + TILE, 2)
    else:
        piece(halo, 0, TILE, 0, 1)
        piece(halo, 0, TILE, RB + TILE, 2)


def run_windows(r, slot, windows):
    @pl.when(r == 0)
    def _():
        for src, halo, buf, sem in windows:
            window_copies(src, halo, buf, sem, r, slot, True)

    @pl.when(r + 1 < NB)
    def _():
        for src, halo, buf, sem in windows:
            window_copies(src, halo, buf, sem, r + 1, 1 - slot, True)

    for src, halo, buf, sem in windows:
        window_copies(src, halo, buf, sem, r, slot, False)


def window_rows(r, ext_rows, far):
    prev = pl.multiple_of(jnp.where(r == 0, ext_rows - TILE, RB * r - TILE), TILE)
    main = pl.multiple_of(RB * r, TILE)
    nxt = pl.multiple_of(jnp.where(r == NB - 1, far, RB * r + RB), TILE)
    return (prev, TILE), (main, RB), (nxt, TILE)


def predict_kernel(u_hbm, v_hbm, p_hbm, ru_hbm, rv_hbm, rp_hbm, re_ref, rw_ref, ku_ref, kv_ref, dzu_ref, dzv_ref,
                   us_out, vs_out, fx_out, fy_out, su_out, sv_out, pw_out, pe_out,
                   ub, vb, pb, kw, ew, q_s, z_s, rhs_u, rhs_v, gu_s, pu_s, gv_s, pv_s, sem):
    r = pl.program_id(0)
    slot = lax.rem(r, 2)
    run_windows(r, slot, [(u_hbm, ru_hbm, ub, sem.at[0]), (v_hbm, rv_hbm, vb, sem.at[1]), (p_hbm, rp_hbm, pb, sem.at[2])])

    at = 0
    for lo, n in window_rows(r, ER, NR):
        for f, ref in enumerate((ku_ref, kv_ref)):
            kw[f, :, at:at + n, :] = ref[:, pl.ds(lo, n), :]
        at += n
    at = 0
    for lo, n in window_rows(r, NR + TILE, NR):
        for f, ref in enumerate((re_ref, rw_ref)):
            ew[f, at:at + n, :] = ref[pl.ds(lo, n), :]
        at += n

    lane48 = lanes_of((48, LANE))

    def tendency(k, _):
        kf = k.astype(F32)
        re, rw = ew[0], ew[1]
        for f, buf in enumerate((ub, vb)):
            for l in range(NP):
                buf[slot, k, l] = jnp.where(kw[f, l] > kf, buf[slot, k, l], ZERO)
            edge = jnp.where(lane48 == 0, roll_to(re, STRIP * f + k, 0), roll_to(rw, STRIP * f + k, LAST))
            buf[slot, k, NP] = jnp.where(kw[f, NP] > kf, edge, ZERO)
        pb[slot, k, NP] = roll_to(re, PAIR + k, 0)
        v0 = [vb[slot, k, l, 0:MID, :] for l in range(NP + 1)]
        v_e = shift_east(v0)
        for l in range(NP + 1):
            q_s[l, 0:MID, :] = (ub[slot, k, l, 0:MID, :] + ub[slot, k, l, 1:41, :]) * (v0[l] + v_e[l])
        for l in range(NP):
            c = vb[slot, k, l, TILE:48, :] + vb[slot, k, l, 7:47, :]
            z_s[l, TILE:48, :] = c * c + pb[slot, k, l, TILE:48, :]
        u0 = [ub[slot, k, l, TILE:MID, :] for l in range(NP + 1)]
        u_w = shift_west(u0)
        w = []
        for l in range(NP + 1):
            c = u0[l] + u_w[l]
            w.append(c * c + pb[slot, k, l, TILE:MID, :])
        w_e = shift_east(w)
        q0 = [q_s[l, TILE:MID, :] for l in range(NP + 1)]
        q_w = shift_west(q0)
        scale = TIME_STEP / 4.0
        for l in range(NP):
            tu = (w_e[l] - w[l]) + (q0[l] - q_s[l, 7:39, :])
            rhs_u[k, l] = jnp.where(kw[0, l, TILE:MID, :] > kf, u0[l] - scale * tu, ZERO)
            tv = (z_s[l, 9:41, :] - z_s[l, TILE:MID, :]) + (q0[l] - q_w[l])
            rhs_v[k, l] = jnp.where(kw[1, l, TILE:MID, :] > kf, vb[slot, k, l, TILE:MID, :] - scale * tv, ZERO)
        return 0

    lax.fori_loop(0, NK, tendency, 0)

    def solve(g, _):
        off = pl.multiple_of(TILE * g, TILE)
        rows = pl.ds(off, TILE)
        wrows = pl.ds(pl.multiple_of(TILE * g + TILE, TILE), TILE)
        grows = pl.ds(pl.multiple_of(RB * r + TILE * g, TILE), TILE)
        ku, kv = kw[0, 0:NP, wrows, :], kw[1, 0:NP, wrows, :]
        dzu, dzv = dzu_ref[0:NP, grows, :], dzv_ref[0:NP, grows, :]

        def coef_of(kf, dz):
            safe = jnp.where(kf > 0, dz, 1.0)
            return (TIME_STEP * VISC_KV) / (safe * safe)

        cu, cv = coef_of(ku, dzu), coef_of(kv, dzv)
        zero = jnp.zeros_like(cu)
        gu, pu, lu, gv, pv, lv = (zero,) * 6
        for k in range(NK):
            upu = jnp.where(ku > k + 1, cu, ZERO) if k < NK - 1 else zero
            upv = jnp.where(kv > k + 1, cv, ZERO) if k < NK - 1 else zero
            iu = 1.0 / ((1.0 + upu + lu) - lu * gu)
            iv = 1.0 / ((1.0 + upv + lv) - lv * gv)
            gu, gv = upu * iu, upv * iv
            pu = (rhs_u[k, :, rows, :] + lu * pu) * iu
            pv = (rhs_v[k, :, rows, :] + lv * pv) * iv
            gu_s[k], pu_s[k], gv_s[k], pv_s[k] = gu, pu, gv, pv
            lu, lv = upu, upv
        bu, bv, su, sv, du, dv = (zero,) * 6
        for k in range(NK - 1, -1, -1):
            bu = pu_s[k] + gu_s[k] * bu
            bv = pv_s[k] + gv_s[k] * bv
            us_out[k, :, rows, :] = bu
            vs_out[k, :, rows, :] = bv
            su = su + bu
            sv = sv + bv
            du = du + (bu - ub[slot, k, 0:NP, wrows, :])
            dv = dv + (bv - vb[slot, k, 0:NP, wrows, :])
        su_out[:, rows, :] = su
        sv_out[:, rows, :] = sv
        fx_out[:, rows, :] = dzu * du * (1.0 / TIME_STEP)
        fy_out[:, rows, :] = dzv * dv * (1.0 / TIME_STEP)
        return 0

    lax.fori_loop(0, RB // TILE, solve, 0)

    lane = lanes_of((RB, LANE))

    def pack(k, acc):
        return jnp.where(lane == PAIR + k, roll_to(us_out[k, NP - 1], LAST, PAIR + k), acc)

    acc = lax.fori_loop(0, NK, pack, jnp.zeros((RB, LANE), F32))
    pw_out[...] = jnp.where(lane < STRIP, fx_out[0], jnp.where(lane < PAIR, pltpu.roll(fy_out[0], STRIP, 1), ZERO))
    pe_out[...] = jnp.where(lane < STRIP, pltpu.roll(fx_out[NP - 1], STRIP, 1), jnp.where(lane < PAIR, pltpu.roll(fy_out[NP - 1], PAIR, 1), acc))


def predict(*args):
    out_cube = pl.BlockSpec((NK, NP, RB, LANE), lambda r: (0, 0, r, 0))
    out_plane = pl.BlockSpec((NP, RB, LANE), lambda r: (0, r, 0))
    edge = pl.BlockSpec((RB, LANE), lambda r: (r, 0))
    window = pltpu.VMEM((2, NK, NP + 1, RB + 16, LANE), F32)
    level = pltpu.VMEM((NP + 1, RB + 16, LANE), F32)
    return pl.pallas_call(
        predict_kernel,
        grid=(NB,),
        in_specs=[ANY] * 6 + [WHOLE] * 6,
        out_specs=[out_cube] * 2 + [out_plane] * 4 + [edge] * 2,
        out_shape=[jax.ShapeDtypeStruct((NK, NP, NR, LANE), F32)] * 2
        + [jax.ShapeDtypeStruct((NP, NR, LANE), F32)] * 4 + [jax.ShapeDtypeStruct((NR, LANE), F32)] * 2,
        scratch_shapes=[window] * 3 + [pltpu.VMEM((2, NP + 1, RB + 16, LANE), F32), pltpu.VMEM((2, RB + 16, LANE), F32), level, level]
        + [pltpu.VMEM((NK, NP, RB, LANE), F32)] * 2 + [pltpu.VMEM((NK, NP, TILE, LANE), F32)] * 4
        + [pltpu.SemaphoreType.DMA((3, 2))],
        compiler_params=pltpu.CompilerParams(vmem_limit_bytes=VMEM_LIMIT),
        name="predict",
    )(*args)


def barotropic_kernel(n_sub, tide_ref, ku_ref, kv_ref, dzu_ref, dzv_ref, kc_ref, eta_ref, tu_ref, tv_ref,
                      fx_ref, fy_ref, su_ref, sv_ref, ref_ref, rwf_ref, rfx_ref, rfy_ref, rvs_ref,
                      eta_out, tu_out, tv_out, cu_out, cv_out,
                      e_s, u_s, v_s, ub_s, vb_s, au_s, bu_s, av_s, bv_s, wet_s):
    dtb = TIME_STEP / n_sub
    weight_norm = 6.0 / (n_sub * (n_sub + 1) * (n_sub + 2))
    planes = range(NP + 1)

    def prepare(c, _):
        base = pl.multiple_of(RB * c, TILE)
        rows = pl.ds(base, RB)
        prow = pl.ds(base + TILE, RB)
        fe, fw = ref_ref[rows, :], rwf_ref[rows, :]

        def forces(l, fx, fy):
            ku, kv = ku_ref[l, rows, :], kv_ref[l, rows, :]
            wu = jnp.where(ku > 0, dtb, ZERO)
            wv = jnp.where(kv > 0, dtb, ZERO)
            au_s[l, rows, :] = wu * (ku * dzu_ref[l, rows, :])
            av_s[l, rows, :] = wv * (kv * dzv_ref[l, rows, :])
            bu_s[l, rows, :] = wu * fx
            bv_s[l, rows, :] = wv * fy

        @pl.when(c < NB)
        def _():
            for l in range(NP):
                forces(l, fx_ref[l, rows, :], fy_ref[l, rows, :])

        @pl.when(c == NB)
        def _():
            for l in range(NP):
                forces(l, rfx_ref[l], rfy_ref[l])

        forces(NP, halo_tile(fe, fw, 0), halo_tile(fe, fw, 1))
        for l in planes:
            wet_s[l, rows, :] = jnp.where(kc_ref[l, rows, :] > 0, dtb, ZERO)
            e_s[l, prow, :] = eta_ref[l, rows, :]
            u_s[l, rows, :] = tu_ref[l, rows, :]
            v_s[l, prow, :] = tv_ref[l, rows, :]
            ub_s[l, rows, :] = jnp.zeros((RB, LANE), F32)
            vb_s[l, rows, :] = jnp.zeros((RB, LANE), F32)
        return 0

    lax.fori_loop(0, ER // RB, prepare, 0)

    def substep(n, _):
        tx, ty = tide_ref[n, 0], tide_ref[n, 1]
        weight = weight_norm * ((n + 1) * (n_sub - n)).astype(F32)
        v_s[:, 0:TILE, :] = v_s[:, ER:ER + TILE, :]
        for c in range(ER // RB):
            b = RB * c
            u0 = [u_s[l, b:b + RB, :] for l in planes]
            u_w = shift_west(u0)
            for l in planes:
                div = (u0[l] - u_w[l]) + (v_s[l, b + TILE:b + TILE + RB, :] - v_s[l, b + 7:b + 7 + RB, :])
                e_s[l, b + TILE:b + TILE + RB, :] = e_s[l, b + TILE:b + TILE + RB, :] - wet_s[l, b:b + RB, :] * div
        e_s[:, ER + TILE:ER + 16, :] = e_s[:, TILE:16, :]
        for c in range(ER // RB):
            b = RB * c
            rows = slice(b, b + RB)
            prow = slice(b + TILE, b + TILE + RB)
            e0 = [e_s[l, prow, :] for l in planes]
            e_e = shift_east(e0)
            for l in planes:
                u = u_s[l, rows, :] + (au_s[l, rows, :] * (tx - (e_e[l] - e0[l])) + bu_s[l, rows, :])
                u_s[l, rows, :] = u
                ub_s[l, rows, :] = ub_s[l, rows, :] + weight * u
                v = v_s[l, prow, :] + (av_s[l, rows, :] * (ty - (e_s[l, b + 9:b + 9 + RB, :] - e0[l])) + bv_s[l, rows, :])
                v_s[l, prow, :] = v
                vb_s[l, rows, :] = vb_s[l, rows, :] + weight * v
        return 0

    lax.fori_loop(0, n_sub, substep, 0)

    def correction(mean, k, dz, total):
        depth = k * dz
        return (mean - dz * total) / jnp.where(depth > 0, depth, 1.0)

    def finish(c, _):
        base = pl.multiple_of(RB * c, TILE)
        rows = pl.ds(base, RB)
        prow = pl.ds(base + TILE, RB)
        for l in range(NP):
            cut = slice(LANE * l, LANE * l + LANE)
            eta_out[rows, cut] = e_s[l, prow, :]
            tu_out[rows, cut] = u_s[l, rows, :]
            tv_out[rows, cut] = v_s[l, prow, :]
            cu_out[l, rows, :] = correction(ub_s[l, rows, :], ku_ref[l, rows, :], dzu_ref[l, rows, :], su_ref[l, rows, :])
            cv_out[l, rows, :] = correction(vb_s[l, rows, :], kv_ref[l, rows, :], dzv_ref[l, rows, :], sv_ref[l, rows, :])
        fw = rwf_ref[rows, :]
        lane = lanes_of(fw.shape)
        total = jnp.sum(jnp.where((lane >= PAIR) & (lane < PAIR + NK), fw, ZERO), axis=1, keepdims=True)
        cu_out[NP, rows, :] = correction(ub_s[NP, rows, :], ku_ref[NP, rows, :], dzu_ref[NP, rows, :], total)
        return 0

    lax.fori_loop(0, NB, finish, 0)
    far = slice(ER - TILE, ER)
    for l in range(NP):
        total = rvs_ref[0, l]
        for k in range(1, NK):
            total = total + rvs_ref[k, l]
        cv_out[l, NR:NR + TILE, :] = correction(vb_s[l, far, :], kv_ref[l, far, :], dzv_ref[l, far, :], total)


def barotropic(tide, *args):
    n_sub = tide.shape[0]
    plane = jax.ShapeDtypeStruct((NR, NX), F32)
    scratch = [pltpu.VMEM((NP + 1, ER + 16, LANE), F32)] * 3 + [pltpu.VMEM((NP + 1, ER, LANE), F32)] * 7
    scratch[1] = pltpu.VMEM((NP + 1, ER, LANE), F32)
    return pl.pallas_call(
        functools.partial(barotropic_kernel, n_sub),
        in_specs=[pl.BlockSpec(memory_space=pltpu.SMEM)] + [WHOLE] * len(args),
        out_specs=[WHOLE] * 5,
        out_shape=[plane] * 3 + [jax.ShapeDtypeStruct((NP + 1, NR, LANE), F32), jax.ShapeDtypeStruct((NP, NR + TILE, LANE), F32)],
        scratch_shapes=scratch,
        compiler_params=pltpu.CompilerParams(vmem_limit_bytes=VMEM_LIMIT),
        name="barotropic",
    )(tide, *args)


def finish_kernel(us_ref, vs_hbm, t_hbm, s_hbm, rvs_hbm, rt_hbm, rs_hbm, rea_ref, rwa_ref, reb_ref, rwf_ref,
                  cu_ref, cv_ref, ku_ref, kv_ref, kc_ref,
                  u_out, v_out, t_out, s_out, vb, tb, sb, kvw, cvw, v_s, sem):
    r = pl.program_id(0)
    slot = lax.rem(r, 2)
    run_windows(r, slot, [(vs_hbm, rvs_hbm, vb, sem.at[0]), (t_hbm, rt_hbm, tb, sem.at[1]), (s_hbm, rs_hbm, sb, sem.at[2])])
    for (lo, n), (lo2, _), at in zip(window_rows(r, ER, NR)[:2], window_rows(r, NR + TILE, NR)[:2], (0, TILE)):
        kvw[:, at:at + n, :] = kv_ref[0:NP, pl.ds(lo, n), :]
        cvw[:, at:at + n, :] = cv_ref[:, pl.ds(lo2, n), :]
    main = pl.ds(pl.multiple_of(RB * r, TILE), RB)
    lane = lanes_of((RB, LANE))
    half = 0.5 * TIME_STEP

    def level(k, _):
        kf = k.astype(F32)
        u = []
        for l in range(NP):
            x = jnp.where(ku_ref[l, main, :] > kf, us_ref[k, l] + cu_ref[l, main, :], ZERO)
            u_out[k, :, LANE * l:LANE * l + LANE] = x
            u.append(half * x)
        x = roll_to(rwf_ref[main, :], PAIR + k, LAST)
        u.append(half * jnp.where(ku_ref[NP, main, :] > kf, x + cu_ref[NP, main, :], ZERO))
        for l in range(NP):
            x = jnp.where(kvw[l] > kf, vb[slot, k, l, 0:MID, :] + cvw[l], ZERO)
            v_out[k, :, LANE * l:LANE * l + LANE] = x[TILE:MID]
            v_s[l] = half * x
        rwa = rwa_ref[main, :]
        t_edge = jnp.where(lane == 0, roll_to(rea_ref[main, :], TAIL + k, 0), roll_to(rwa, PAIR + k, LAST))
        s_edge = jnp.where(lane == 0, roll_to(reb_ref[main, :], STRIP + k, 0), roll_to(rwa, TAIL + k, LAST))
        for buf, edge, out in ((tb, t_edge, t_out), (sb, s_edge, s_out)):
            x0 = [buf[slot, k, l, TILE:MID, :] for l in range(NP)] + [edge]
            x_e = shift_east(x0)
            fx = [u[l] * (x0[l] + x_e[l]) for l in range(NP + 1)]
            fx_w = shift_west(fx)
            for l in range(NP):
                fy = v_s[l, TILE:MID, :] * (x0[l] + buf[slot, k, l, 9:41, :])
                fy_s = v_s[l, 7:39, :] * (buf[slot, k, l, 7:39, :] + x0[l])
                new = x0[l] - ((fx[l] - fx_w[l]) + (fy - fy_s))
                out[k, :, LANE * l:LANE * l + LANE] = jnp.where(kc_ref[l, main, :] > kf, new, ZERO)
        return 0

    lax.fori_loop(0, NK, level, 0)


def finish(*args):
    cube = pl.BlockSpec((NK, NP, RB, LANE), lambda r: (0, 0, r, 0))
    out_cube = pl.BlockSpec((NK, RB, NX), lambda r: (0, r, 0))
    window = pltpu.VMEM((2, NK, NP, RB + 16, LANE), F32)
    return pl.pallas_call(
        finish_kernel,
        grid=(NB,),
        in_specs=[cube] + [ANY] * 6 + [WHOLE] * 9,
        out_specs=[out_cube] * 4,
        out_shape=[jax.ShapeDtypeStruct((NK, NR, NX), F32)] * 4,
        scratch_shapes=[window] * 3 + [pltpu.VMEM((NP, MID, LANE), F32)] * 3 + [pltpu.SemaphoreType.DMA((3, 2))],
        compiler_params=pltpu.CompilerParams(vmem_limit_bytes=VMEM_LIMIT),
        name="finish",
    )(*args)


def solution(mesh):
    n_cols = mesh.shape["col"]

    def shape(*dims, dtype=F32):
        return jax.ShapeDtypeStruct(dims, dtype)

    def local_step(vel_u, vel_v, temp, salt, eta, trans_u, trans_v, depth, kmt, tide):
        p4, t_mix, s_mix, ewa, eea, ewb, eeb, p1w, p1e = mix(vel_u, vel_v, temp, salt, eta, trans_u, trans_v, depth, kmt)
        plan = [("west", 0, 0, TILE), ("east", 1, 1, TILE), ("west", 2, 2, STRIP), ("east", 3, 3, STRIP), ("west", 4, 4, STRIP), ("east", 5, 5, STRIP)]
        plan += [("rows2", 6 + n, 6 + n, STRIP) for n in range(5)]
        plan += [("rows3", 11, 11, TILE), ("rows3", 12, 12, TILE)] + [("rows4", 13 + n, 13 + n, TILE) for n in range(3)]
        ins = [ewa, eea, ewb, eeb, p1w, p1e, kmt, depth, eta, trans_u, trans_v, vel_u, vel_v, p4, t_mix, s_mix]
        outs = [shape(NR + TILE, LANE)] * 2 + [shape(ER, LANE)] * 4 + [shape(HALO, NX, dtype=jnp.int32)] + [shape(HALO, NX)] * 4
        outs += [shape(NK, TILE, NX)] * 2 + [shape(NK, NP, TILE, LANE)] * 3
        rea, rwa, reb, rwb, rep, rwp, rk, rh, reta, rtu, rtv, ru, rv, rp, rt, rs = exchange(n_cols, plan, ins, outs, 0)
        ku, kv, dzu, dzv, kc, eta_x, tu_x, tv_x = geometry(kmt, depth, eta, trans_u, trans_v, rep, rwp, reb, rwb, rk, rh, reta, rtu, rtv)
        us, vs, fx, fy, su, sv, pw, pe = predict(vel_u, vel_v, p4, ru, rv, rp, rea, rwa, ku, kv, dzu, dzv)
        plan = [("west", 0, 0, STRIP), ("east", 1, 1, STRIP), ("rows3", 2, 2, STRIP), ("rows3", 3, 3, STRIP), ("rows4", 4, 4, TILE)]
        outs = [shape(ER, LANE)] * 2 + [shape(NP, HALO, LANE)] * 2 + [shape(NK, NP, TILE, LANE)]
        ref, rwf, rfx, rfy, rvs = exchange(n_cols, plan, [pw, pe, fx, fy, vs], outs, 1)
        eta_new, tu_new, tv_new, cu, cv = barotropic(tide, ku, kv, dzu, dzv, kc, eta_x, tu_x, tv_x, fx, fy, su, sv, ref, rwf, rfx, rfy, rvs)
        u_new, v_new, t_new, s_new = finish(us, vs, t_mix, s_mix, rvs, rt, rs, rea, rwa, reb, rwf, cu, cv, ku, kv, kc)
        return eta_new, tu_new, tv_new, u_new, v_new, t_new, s_new

    cube = P(None, "row", "col")
    plane = P("row", "col")
    return jax.shard_map(local_step, mesh=mesh, in_specs=(cube,) * 4 + (plane,) * 5 + (P(None, None),), out_specs=(plane,) * 3 + (cube,) * 4, check_vma=False)
```
